512 devices in a mesh: trial: 4 (over y), time: 32 (over z, core), chan: 4 (over x).
Axes of the slice: x: 4, y: 4, z: 16, core: 2. Of those that a mesh axis runs over, the one named last changes fastest.
Arguments:
- fade_rate: float32 [4, 8192, 2560], P('trial', 'time', 'chan'), parts along dimension 0, may hold values from 0.2 to 2
- update_in: bfloat16 [4, 8192, 2560], P('trial', 'time', 'chan'), parts along dimension 0, may hold values from -6 to 6
- gate_in: bfloat16 [4, 8192, 2560], P('trial', 'time', 'chan'), parts along dimension 0, may hold values from -6 to 6
- norm_gain: float32 [10240], P(('trial', 'chan')), parts along dimension 0, may hold values from 0.25 to 1.75
Outputs:
- sequence_out: bfloat16 [4, 8192, 2560], P('trial', 'time', 'chan'), parts along dimension 0
The draws below stay inside these ranges and needn't reach their ends.
There are 4 independent parts, one for each index of `trial`. The reference program is written for one: setup_inputs(seed, part) draws one part's arguments, and reference() takes and returns one part's arrays. A program takes and returns all parts, laid end to end along the dimension named above; each array names one. Nothing has to cross between parts.
All inputs are finite; a program needn't handle non-finite values.
Results may differ from the reference program's by a relative error of at most 0.001.
Values sent between devices are 32-bit elements; how exact they have to be, the bound alone decides.
No kernel may reach another device: no remote copies, remote signals or barrier semaphores. Data moves between devices by JAX's collectives and lax.ppermute only.
A program may use at most 64 MiB of HBM per device.

```python
import jax
import jax.numpy as jnp
from jax import lax

BATCH = 1
CHANNELS = 2560
LENGTH = 8192


def block_scale(rng, shape, shards, smallest, top_value):
    level, own = 1.0, jax.random.fold_in(rng, 6)
    for axis_at, shards_of in shards:
        steps = jnp.exp(jax.random.uniform(jax.random.fold_in(own, axis_at), (shards_of,), jnp.float32, smallest / len(shards), top_value / len(shards)))
        level = level * jnp.repeat(steps, shape[axis_at] // shards_of).reshape([-1 if axis == axis_at else 1 for axis in range(len(shape))])
    return level


def bell_draw(key, extent, deviation, reach, split=(), dtype=jnp.bfloat16):
    result = jax.random.normal(key, extent, jnp.float32) * deviation
    if len(split) > 0:
        result = block_scale(key, extent, split, -0.22, 0.18) * result
    return jnp.clip(result, min=-reach, max=reach).astype(dtype)


def setup_inputs(seed: int = 0, part: int = 0) -> dict:
    streams_of = jax.random.split(jax.random.key(seed), 5)
    own_keys = jax.random.split(jax.random.fold_in(streams_of[4], part), 5)
    fade_rate = jnp.clip(0.2 + 1.8 * jax.random.uniform(own_keys[0], (BATCH, LENGTH, CHANNELS), jnp.float32) ** block_scale(own_keys[0], (BATCH, LENGTH, CHANNELS), ((1, 32), (2, 4)), -0.2, 0.2), 0.2, 2.0)
    update_in = bell_draw(own_keys[1], (BATCH, LENGTH, CHANNELS), 1.0, 6.0, ((1, 32), (2, 4)))
    gate_in = bell_draw(own_keys[2], (BATCH, LENGTH, CHANNELS), 1.0, 6.0, ((1, 32), (2, 4)))
    norm_gain = jnp.clip(1.0 + 0.15 * jax.random.normal(own_keys[3], (CHANNELS,), jnp.float32), 0.25, 1.75)
    return dict(fade_rate=fade_rate, update_in=update_in, gate_in=gate_in, norm_gain=norm_gain)


def join_pair(earlier, later):
    return (earlier[0] * later[0], later[0] * earlier[1] + later[1])

def reference(fade_rate, update_in, gate_in, norm_gain):
    keep = jnp.exp(-fade_rate / LENGTH)
    push = update_in.astype(jnp.float32) * LENGTH ** (-0.5)
    forward = lax.associative_scan(join_pair, (keep, push), axis=1)[1]
    backward = lax.associative_scan(join_pair, (keep, push), axis=1, reverse=True)[1]
    states = forward + backward
    gated = states * jax.nn.sigmoid(gate_in.astype(jnp.float32))
    power = lax.optimization_barrier(jnp.mean(gated * gated, axis=-1, keepdims=True))
    sequence_out = (gated * lax.rsqrt(power + 1e-06) * norm_gain).astype(jnp.bfloat16)
    return sequence_out
```

```python
import functools

import jax
import jax.numpy as jnp
from jax import lax
from jax.experimental import pallas as pl
from jax.experimental.pallas import tpu as pltpu
from jax.sharding import Mesh
from jax.sharding import PartitionSpec as P

CHUNKS = ((0, 256), (256, 384))
SHIFT = 8


def dot_split(left, right):
    high = right.astype(jnp.bfloat16)
    low = (right - high.astype(jnp.float32)).astype(jnp.bfloat16)
    return jnp.dot(left, high, preferred_element_type=jnp.float32) + jnp.dot(
        left, low, preferred_element_type=jnp.float32
    )


def triangle(size, upper):
    row = lax.broadcasted_iota(jnp.int32, (size, size), 0)
    col = lax.broadcasted_iota(jnp.int32, (size, size), 1)
    keep = (col >= row) if upper else (col <= row)
    return keep.astype(jnp.float32).astype(jnp.bfloat16)


def copies(sources, targets, sems):
    rows = []
    for k, (at, width) in enumerate(CHUNKS):
        rows.append(
            [
                pltpu.make_async_copy(
                    s.at[:, pl.ds(at, width)], t.at[:, pl.ds(at, width)], sems.at[k, n]
                )
                for n, (s, t) in enumerate(zip(sources, targets))
            ]
        )
    for row in rows:
        for copy in row:
            copy.start()
    return rows


def summary_kernel(total, fade_hbm, push_hbm, out, fade, push, sems):
    rows = copies((fade_hbm, push_hbm), (fade, push), sems)
    lower = triangle(fade.shape[0], False)
    for (at, width), row in zip(CHUNKS, rows):
        for copy in row:
            copy.wait()
        cols = pl.ds(at, width)
        rate = fade[:, cols] * (1.0 / total)
        value = push[:, cols].astype(jnp.float32)
        run = dot_split(lower, rate)
        all_of = jnp.sum(rate, axis=0, keepdims=True)
        product = jnp.exp(-all_of)
        scale = total ** (-0.5)
        out[0:1, cols] = product
        out[1:2, cols] = (
            product * scale * jnp.sum(jnp.exp(run) * value, axis=0, keepdims=True)
        )
        out[2:3, cols] = scale * jnp.sum(jnp.exp(rate - run) * value, axis=0, keepdims=True)


def chip_kernel(both, out):
    place = lax.axis_index("z")
    p0, f0, b0 = (both[0, k : k + 1, :] for k in range(3))
    p1, f1, b1 = (both[1, k : k + 1, :] for k in range(3))
    product = p0 * p1
    forward = f1 + p1 * f0
    backward = b0 + p0 * b1
    count = out.shape[0]
    for k in range(count):
        out[k, 0:1, :] = product
        out[k, 1:2, :] = jnp.where(place < (k + SHIFT) % count, forward, backward)


def local_kernel(
    total, fade_hbm, push_hbm, gate_hbm, after, own, first, second, fade, push, gate, sems
):
    del after
    rows = copies((fade_hbm, push_hbm, gate_hbm), (fade, push, gate), sems)
    lower = triangle(fade.shape[0], False)
    upper = triangle(fade.shape[0], True)
    for (at, width), row in zip(CHUNKS, rows):
        for copy in row:
            copy.wait()
        cols = pl.ds(at, width)
        rate = fade[:, cols] * (1.0 / total)
        value = push[:, cols].astype(jnp.float32) * total ** (-0.5)
        gated = 1.0 / (1.0 + jnp.exp(-gate[:, cols].astype(jnp.float32)))
        run = dot_split(lower, rate)
        down = jnp.exp(-run)
        up = jnp.exp(run - rate)
        ahead = dot_split(lower, jnp.exp(run) * value)
        behind = dot_split(upper, jnp.exp(rate - run) * value)
        first[:, cols] = down * gated
        second[:, cols] = up * gated
        own[:, cols] = (down * ahead + up * behind) * gated


def join_kernel(both, others, own, first, second, gated, power):
    place, core = lax.axis_index("z"), lax.axis_index("core")
    count = others.shape[0]
    ahead = jnp.zeros_like(both[0, 0:1, :])
    behind = jnp.zeros_like(ahead)
    for k in range(count):
        at = (k + count - SHIFT) % count
        ahead = jnp.where(k < place, others[at, 0:1, :] * ahead + others[at, 1:2, :], ahead)
        j = count - 1 - k
        at = (j + count - SHIFT) % count
        behind = jnp.where(j > place, others[at, 0:1, :] * behind + others[at, 1:2, :], behind)
    p0, f0 = both[0, 0:1, :], both[0, 1:2, :]
    p1, b1 = both[1, 0:1, :], both[1, 2:3, :]
    low = core == 0
    ahead = jnp.where(low, ahead, f0 + p0 * ahead)
    behind = jnp.where(low, p0 * (b1 + p1 * behind), p1 * behind)
    lane = lax.broadcasted_iota(jnp.int32, (8, 128), 1)
    sums = jnp.zeros((8, 128), jnp.float32)
    for i in range(own.shape[0] // 8):
        rows = slice(8 * i, 8 * i + 8)
        value = own[rows, :] + first[rows, :] * ahead + second[rows, :] * behind
        gated[rows, :] = value
        part = jnp.sum(value * value, axis=1, keepdims=True)
        sums = jnp.where(lane == i, part, sums)
    for k in range(power.shape[0]):
        power[k] = sums


def norm_kernel(channels, powers, gated, gain, out_hbm, out, sems):
    power = powers[0] + powers[1] + powers[2] + powers[3]
    root = lax.rsqrt(power * (1.0 / channels) + 1e-06)
    weight = gain[...]
    count, pieces = out.shape[0] // 16, []
    for i in range(count):
        rows = slice(16 * i, 16 * i + 16)
        r = jnp.concatenate([root[:, 2 * i : 2 * i + 1], root[:, 2 * i + 1 : 2 * i + 2]], axis=0)
        out[rows, :] = (gated[rows, :] * r * weight).astype(jnp.bfloat16)
        if (i + 1) % (count // 2) == 0:
            half = (i + 1) // (count // 2) - 1
            size = out.shape[0] // 2
            piece = pltpu.make_async_copy(
                out.at[pl.ds(half * size, size), :],
                out_hbm.at[pl.ds(half * size, size), :],
                sems.at[half],
            )
            piece.start()
            pieces.append(piece)
    for piece in pieces:
        piece.wait()


ANY = pl.BlockSpec(memory_space=pl.ANY)
VMEM = pl.BlockSpec(memory_space=pltpu.VMEM)


def shape_of(*shape, dtype=jnp.float32):
    return jax.ShapeDtypeStruct(shape, dtype)


def per_device(fade_rate, update_in, gate_in, norm_gain):
    fade_rate, update_in, gate_in = fade_rate[0], update_in[0], gate_in[0]
    length, width = fade_rate.shape
    chips, chans = lax.axis_size("z"), lax.axis_size("chan")
    total = float(length * chips * lax.axis_size("core"))
    params = pltpu.CompilerParams(vmem_limit_bytes=16 * 2**20)
    f32, bf16 = jnp.float32, jnp.bfloat16
    block = (length, width)
    summary = pl.pallas_call(
        functools.partial(summary_kernel, total),
        out_shape=shape_of(3, width),
        in_specs=[ANY, ANY],
        out_specs=VMEM,
        scratch_shapes=[
            pltpu.VMEM(block, f32),
            pltpu.VMEM(block, bf16),
            pltpu.SemaphoreType.DMA((len(CHUNKS), 2)),
        ],
        compiler_params=params,
        name="summary",
    )(fade_rate, update_in)
    both = lax.all_gather(summary, "core")
    sent = pl.pallas_call(
        chip_kernel,
        out_shape=shape_of(chips, 2, width),
        in_specs=[VMEM],
        out_specs=VMEM,
        compiler_params=params,
        name="chip",
    )(both)
    order = [[(k + SHIFT) % chips for k in range(chips)]]
    others = lax.all_to_all(sent, "z", 0, 0, axis_index_groups=order, tiled=True)
    own, first, second = pl.pallas_call(
        functools.partial(local_kernel, total),
        out_shape=[shape_of(*block)] * 3,
        in_specs=[ANY] * 4,
        out_specs=[VMEM] * 3,
        scratch_shapes=[
            pltpu.VMEM(block, f32),
            pltpu.VMEM(block, bf16),
            pltpu.VMEM(block, bf16),
            pltpu.SemaphoreType.DMA((len(CHUNKS), 3)),
        ],
        compiler_params=params,
        cost_estimate=pl.CostEstimate(
            flops=1_000_000_000, bytes_accessed=4_000_000, transcendentals=1_000_000
        ),
        name="local",
    )(fade_rate, update_in, gate_in, sent)
    gated, power = pl.pallas_call(
        join_kernel,
        out_shape=[shape_of(*block), shape_of(chans, 8, 128)],
        in_specs=[VMEM] * 5,
        out_specs=[VMEM] * 2,
        compiler_params=params,
        name="join",
    )(both, others, own, first, second)
    powers = lax.all_to_all(power, "chan", 0, 0, tiled=True)
    out = pl.pallas_call(
        functools.partial(norm_kernel, float(width * chans)),
        out_shape=shape_of(*block, dtype=bf16),
        in_specs=[VMEM] * 3,
        out_specs=ANY,
        scratch_shapes=[pltpu.VMEM(block, bf16), pltpu.SemaphoreType.DMA((2,))],
        compiler_params=params,
        name="norm",
    )(powers, gated, norm_gain.reshape(1, width))
    return out[None]


def solution(mesh):
    torus = Mesh(
        mesh.devices.reshape(mesh.shape["trial"], mesh.shape["time"] // 2, 2, mesh.shape["chan"]),
        ("trial", "z", "core", "chan"),
    )
    time = ("z", "core")
    spec = P("trial", time, "chan")
    return jax.shard_map(
        per_device,
        mesh=torus,
        in_specs=(spec, spec, spec, P(("trial", "chan"))),
        out_specs=spec,
        check_vma=False,
    )
```

```python
import functools

import jax
import jax.numpy as jnp
from jax import lax
from jax.experimental import pallas as pl
from jax.experimental.pallas import tpu as pltpu
from jax.sharding import Mesh
from jax.sharding import PartitionSpec as P

CHUNKS = ((0, 384), (384, 256))
ORDER = (11, 12, 13, 14, 15, 0, 1, 2, 3, 4, 5, 6, 7, 8, 9, 10)
PIECES = 4
CHAN_ORDER = (2, 1, 0, 3)
EARLY = 3


def dot_split(left, right):
    high = right.astype(jnp.bfloat16)
    low = (right - high.astype(jnp.float32)).astype(jnp.bfloat16)
    return jnp.dot(left, high, preferred_element_type=jnp.float32) + jnp.dot(
        left, low, preferred_element_type=jnp.float32
    )


def triangle(size, upper):
    row = lax.broadcasted_iota(jnp.int32, (size, size), 0)
    col = lax.broadcasted_iota(jnp.int32, (size, size), 1)
    keep = (col >= row) if upper else (col <= row)
    return keep.astype(jnp.float32).astype(jnp.bfloat16)


def copies(sources, targets, sems):
    rows = []
    for k, (at, width) in enumerate(CHUNKS):
        rows.append(
            [
                pltpu.make_async_copy(
                    s.at[:, pl.ds(at, width)], t.at[:, pl.ds(at, width)], sems.at[k, n]
                )
                for n, (s, t) in enumerate(zip(sources, targets))
            ]
        )
    for row in rows:
        for copy in row:
            copy.start()
    return rows


def summary_kernel(
    total, fade_hbm, push_hbm, gate_hbm, gain_hbm, out, fade, push, gate, gain, sems, late_sems
):
    rows = copies((fade_hbm, push_hbm), (fade, push), sems)
    late = [
        pltpu.make_async_copy(gate_hbm, gate, late_sems.at[0]),
        pltpu.make_async_copy(gain_hbm, gain, late_sems.at[1]),
    ]
    for copy in late:
        copy.start()
    lower = triangle(fade.shape[0], False)
    for (at, width), row in zip(CHUNKS, rows):
        for copy in row:
            copy.wait()
        cols = pl.ds(at, width)
        rate = fade[:, cols] * (1.0 / total)
        value = push[:, cols].astype(jnp.float32)
        run = dot_split(lower, rate)
        all_of = jnp.sum(rate, axis=0, keepdims=True)
        product = jnp.exp(-all_of)
        scale = total ** (-0.5)
        out[0:1, cols] = product
        out[1:2, cols] = (
            product * scale * jnp.sum(jnp.exp(run) * value, axis=0, keepdims=True)
        )
        out[2:3, cols] = scale * jnp.sum(jnp.exp(rate - run) * value, axis=0, keepdims=True)
    for copy in late:
        copy.wait()


def local_parts(total, lower, upper, fade, push, gate, cols):
    rate = fade[:, cols] * (1.0 / total)
    value = push[:, cols].astype(jnp.float32) * total ** (-0.5)
    run = dot_split(lower, rate)
    down = jnp.exp(-run)
    up = jnp.exp(run - rate)
    ahead = dot_split(lower, jnp.exp(run) * value)
    behind = dot_split(upper, jnp.exp(rate - run) * value)
    share = 1.0 / (1.0 + jnp.exp(-gate[:, cols].astype(jnp.float32)))
    return down, up, ahead, behind, share


def chip_kernel(total, both, fade, push, gate, out, own, first, second):
    place = lax.axis_index("z")
    p0, f0, b0 = (both[0, k : k + 1, :] for k in range(3))
    p1, f1, b1 = (both[1, k : k + 1, :] for k in range(3))
    product = p0 * p1
    forward = f1 + p1 * f0
    backward = b0 + p0 * b1
    count = out.shape[0]
    for k in range(count):
        out[k, 0:1, :] = product
        out[k, 1:2, :] = jnp.where(place < ORDER[k], forward, backward)

    @pl.when(place < EARLY)
    def _():
        lower, upper = triangle(fade.shape[0], False), triangle(fade.shape[0], True)
        for at, width in CHUNKS:
            cols = pl.ds(at, width)
            down, up, ahead, behind, share = local_parts(
                total, lower, upper, fade, push, gate, cols
            )
            first[:, cols] = down * share
            second[:, cols] = up * share
            own[:, cols] = (down * ahead + up * behind) * share


def join_kernel(
    total, both, others, fade, push, gate, own, first, second, gain, gated, power, ends, total_sum
):
    place, core = lax.axis_index("z"), lax.axis_index("core")
    count = others.shape[0]
    ahead = jnp.zeros_like(both[0, 0:1, :])
    behind = jnp.zeros_like(ahead)
    for k in range(count):
        at = ORDER.index(k)
        ahead = jnp.where(k < place, others[at, 0:1, :] * ahead + others[at, 1:2, :], ahead)
        j = count - 1 - k
        at = ORDER.index(j)
        behind = jnp.where(j > place, others[at, 0:1, :] * behind + others[at, 1:2, :], behind)
    p0, f0 = both[0, 0:1, :], both[0, 1:2, :]
    p1, b1 = both[1, 0:1, :], both[1, 2:3, :]
    low = core == 0
    ends[0:1, :] = jnp.where(low, ahead, f0 + p0 * ahead)
    ends[1:2, :] = jnp.where(low, p0 * (b1 + p1 * behind), p1 * behind)
    for k in range(gain.shape[0] // 128):
        cols = pl.ds(128 * k, 128)
        ends[2:3, cols] = gain[cols].reshape(1, 128)
    lane = lax.broadcasted_iota(jnp.int32, (8, 128), 1)
    length = own.shape[0]

    @pl.when(place < EARLY)
    def _():
        ahead, behind, weight = ends[0:1, :], ends[1:2, :], ends[2:3, :]
        sums = jnp.zeros((8, 128), jnp.float32)
        for i in range(length // 8):
            rows = slice(8 * i, 8 * i + 8)
            value = own[rows, :] + first[rows, :] * ahead + second[rows, :] * behind
            gated[rows, :] = value * weight
            part = jnp.sum(value * value, axis=1, keepdims=True)
            sums = jnp.where(lane == i, part, sums)
        total_sum[...] = sums

    @pl.when(place >= EARLY)
    def _():
        lower, upper = triangle(length, False), triangle(length, True)
        squares = jnp.zeros((length, 128), jnp.float32)
        for at, width in CHUNKS:
            cols = pl.ds(at, width)
            down, up, mine, rest, share = local_parts(
                total, lower, upper, fade, push, gate, cols
            )
            value = (down * (mine + ends[0:1, cols]) + up * (rest + ends[1:2, cols])) * share
            gated[:, cols] = value * ends[2:3, cols]
            value = value * value
            for k in range(width // 128):
                squares = squares + value[:, 128 * k : 128 * k + 128]
        sums = jnp.zeros((8, 128), jnp.float32)
        for i in range(length // 8):
            part = jnp.sum(squares[8 * i : 8 * i + 8, :], axis=1, keepdims=True)
            sums = jnp.where(lane == i, part, sums)
        total_sum[...] = sums

    for k in range(power.shape[0]):
        power[k] = total_sum[...]


def norm_kernel(channels, powers, gated, out_hbm, out, sems):
    power = powers[0] + powers[1] + powers[2] + powers[3]
    root = lax.rsqrt(power * (1.0 / channels) + 1e-06)
    count, pieces = out.shape[0] // 16, []
    for i in range(count):
        rows = slice(16 * i, 16 * i + 16)
        r = jnp.concatenate([root[:, 2 * i : 2 * i + 1], root[:, 2 * i + 1 : 2 * i + 2]], axis=0)
        out[rows, :] = (gated[rows, :] * r).astype(jnp.bfloat16)
        if (i + 1) % (count // PIECES) == 0:
            half = (i + 1) // (count // PIECES) - 1
            size = out.shape[0] // PIECES
            piece = pltpu.make_async_copy(
                out.at[pl.ds(half * size, size), :],
                out_hbm.at[pl.ds(half * size, size), :],
                sems.at[half],
            )
            piece.start()
            pieces.append(piece)
    for piece in pieces:
        piece.wait()


ANY = pl.BlockSpec(memory_space=pl.ANY)
HBM = pl.BlockSpec(memory_space=pltpu.HBM)
VMEM = pl.BlockSpec(memory_space=pltpu.VMEM)


def shape_of(*shape, dtype=jnp.float32):
    return jax.ShapeDtypeStruct(shape, dtype)


def in_hbm(value):
    return pltpu.with_memory_space_constraint(value, pltpu.HBM)


def per_device(fade_rate, update_in, gate_in, norm_gain):
    fade_rate, update_in, gate_in = fade_rate[0], update_in[0], gate_in[0]
    length, width = fade_rate.shape
    chips, chans = lax.axis_size("z"), lax.axis_size("chan")
    total = float(length * chips * lax.axis_size("core"))
    params = pltpu.CompilerParams(vmem_limit_bytes=16 * 2**20)
    f32, bf16 = jnp.float32, jnp.bfloat16
    block = (length, width)
    summary, fade, push, gate, gain = pl.pallas_call(
        functools.partial(summary_kernel, total),
        out_shape=[
            shape_of(3, width),
            shape_of(*block),
            shape_of(*block, dtype=bf16),
            shape_of(*block, dtype=bf16),
            shape_of(width),
        ],
        in_specs=[HBM] * 4,
        out_specs=[VMEM] * 5,
        scratch_shapes=[
            pltpu.SemaphoreType.DMA((len(CHUNKS), 2)),
            pltpu.SemaphoreType.DMA((2,)),
        ],
        compiler_params=params,
        name="summary",
    )(in_hbm(fade_rate), in_hbm(update_in), in_hbm(gate_in), in_hbm(norm_gain))
    both = lax.all_gather(summary, "core")
    sent, own, first, second = pl.pallas_call(
        functools.partial(chip_kernel, total),
        out_shape=[shape_of(chips, 2, width)] + [shape_of(*block)] * 3,
        in_specs=[VMEM] * 4,
        out_specs=[VMEM] * 4,
        compiler_params=params,
        name="chip",
    )(both, fade, push, gate)
    others = lax.all_to_all(sent, "z", 0, 0, axis_index_groups=[list(ORDER)], tiled=True)
    gated, power = pl.pallas_call(
        functools.partial(join_kernel, total),
        out_shape=[shape_of(*block), shape_of(chans, 8, 128)],
        in_specs=[VMEM] * 9,
        out_specs=[VMEM] * 2,
        scratch_shapes=[pltpu.VMEM((3, width), f32), pltpu.VMEM((8, 128), f32)],
        compiler_params=params,
        name="join",
    )(both, others, fade, push, gate, own, first, second, gain)
    powers = lax.all_to_all(
        power, "chan", 0, 0, axis_index_groups=[list(CHAN_ORDER)], tiled=True
    )
    out = pl.pallas_call(
        functools.partial(norm_kernel, float(width * chans)),
        out_shape=shape_of(*block, dtype=bf16),
        in_specs=[VMEM] * 2,
        out_specs=ANY,
        scratch_shapes=[pltpu.VMEM(block, bf16), pltpu.SemaphoreType.DMA((PIECES,))],
        compiler_params=params,
        name="norm",
    )(powers, gated)
    return out[None]


def solution(mesh):
    torus = Mesh(
        mesh.devices.reshape(mesh.shape["trial"], mesh.shape["time"] // 2, 2, mesh.shape["chan"]),
        ("trial", "z", "core", "chan"),
    )
    time = ("z", "core")
    spec = P("trial", time, "chan")
    return jax.shard_map(
        per_device,
        mesh=torus,
        in_specs=(spec, spec, spec, P(("trial", "chan"))),
        out_specs=spec,
        check_vma=False,
    )
```

```python
import functools

import jax
import jax.numpy as jnp
from jax import lax
from jax.experimental import pallas as pl
from jax.experimental.pallas import tpu as pltpu
from jax.sharding import Mesh
from jax.sharding import PartitionSpec as P

CHUNKS = ((0, 384), (384, 256))
ORDER = (11, 12, 13, 14, 15, 0, 1, 2, 3, 4, 5, 6, 7, 8, 9, 10)
PIECES = 4
CHAN_ORDER = (2, 1, 0, 3)
EARLY = 3
NEAR = (0, 1, 2)


def dot_split(left, right):
    high = right.astype(jnp.bfloat16)
    low = (right - high.astype(jnp.float32)).astype(jnp.bfloat16)
    return jnp.dot(left, high, preferred_element_type=jnp.float32) + jnp.dot(
        left, low, preferred_element_type=jnp.float32
    )


def triangle(size, upper):
    row = lax.broadcasted_iota(jnp.int32, (size, size), 0)
    col = lax.broadcasted_iota(jnp.int32, (size, size), 1)
    keep = (col >= row) if upper else (col <= row)
    return keep.astype(jnp.float32).astype(jnp.bfloat16)


def copies(sources, targets, sems):
    rows = []
    for k, (at, width) in enumerate(CHUNKS):
        rows.append(
            [
                pltpu.make_async_copy(
                    s.at[:, pl.ds(at, width)], t.at[:, pl.ds(at, width)], sems.at[k, n]
                )
                for n, (s, t) in enumerate(zip(sources, targets))
            ]
        )
    for row in rows:
        for copy in row:
            copy.start()
    return rows


def summary_kernel(
    total, fade_hbm, push_hbm, gate_hbm, gain_hbm, out, fade, push, gate, gain, sems, late_sems
):
    rows = copies((fade_hbm, push_hbm), (fade, push), sems)
    late = [
        pltpu.make_async_copy(gate_hbm, gate, late_sems.at[0]),
        pltpu.make_async_copy(gain_hbm, gain, late_sems.at[1]),
    ]
    for copy in late:
        copy.start()
    lower = triangle(fade.shape[0], False)
    for (at, width), row in zip(CHUNKS, rows):
        for copy in row:
            copy.wait()
        cols = pl.ds(at, width)
        rate = fade[:, cols] * (1.0 / total)
        value = push[:, cols].astype(jnp.float32)
        run = dot_split(lower, rate)
        all_of = jnp.sum(rate, axis=0, keepdims=True)
        product = jnp.exp(-all_of)
        scale = total ** (-0.5)
        out[0:1, cols] = product
        out[1:2, cols] = (
            product * scale * jnp.sum(jnp.exp(run) * value, axis=0, keepdims=True)
        )
        out[2:3, cols] = scale * jnp.sum(jnp.exp(rate - run) * value, axis=0, keepdims=True)
    for copy in late:
        copy.wait()


def local_parts(total, lower, upper, fade, push, gate, cols):
    rate = fade[:, cols] * (1.0 / total)
    value = push[:, cols].astype(jnp.float32) * total ** (-0.5)
    run = dot_split(lower, rate)
    down = jnp.exp(-run)
    up = jnp.exp(run - rate)
    ahead = dot_split(lower, jnp.exp(run) * value)
    behind = dot_split(upper, jnp.exp(rate - run) * value)
    share = 1.0 / (1.0 + jnp.exp(-gate[:, cols].astype(jnp.float32)))
    return down, up, ahead, behind, share


def chip_kernel(total, both, fade, push, gate, out, own, first, second):
    place = lax.axis_index("z")
    p0, f0, b0 = (both[0, k : k + 1, :] for k in range(3))
    p1, f1, b1 = (both[1, k : k + 1, :] for k in range(3))
    product = p0 * p1
    forward = f1 + p1 * f0
    backward = b0 + p0 * b1
    count = out.shape[0]
    for k in range(count):
        out[k, 0:1, :] = product
        out[k, 1:2, :] = jnp.where(place < ORDER[k], forward, backward)

    @pl.when(place < EARLY)
    def _():
        lower, upper = triangle(fade.shape[0], False), triangle(fade.shape[0], True)
        for at, width in CHUNKS:
            cols = pl.ds(at, width)
            down, up, ahead, behind, share = local_parts(
                total, lower, upper, fade, push, gate, cols
            )
            first[:, cols] = down * share
            second[:, cols] = up * share
            own[:, cols] = (down * ahead + up * behind) * share


def join_kernel(
    total, both, others, fade, push, gate, own, first, second, gain, gated, power, ends, total_sum
):
    place, core = lax.axis_index("z"), lax.axis_index("core")
    count = others.shape[0]
    ahead = jnp.zeros_like(both[0, 0:1, :])
    behind = jnp.zeros_like(ahead)
    for k in range(count):
        at = ORDER.index(k)
        ahead = jnp.where(k < place, others[at, 0:1, :] * ahead + others[at, 1:2, :], ahead)
        j = count - 1 - k
        at = ORDER.index(j)
        behind = jnp.where(j > place, others[at, 0:1, :] * behind + others[at, 1:2, :], behind)
    p0, f0 = both[0, 0:1, :], both[0, 1:2, :]
    p1, b1 = both[1, 0:1, :], both[1, 2:3, :]
    low = core == 0
    ends[0:1, :] = jnp.where(low, ahead, f0 + p0 * ahead)
    ends[1:2, :] = jnp.where(low, p0 * (b1 + p1 * behind), p1 * behind)
    for k in range(gain.shape[0] // 128):
        cols = pl.ds(128 * k, 128)
        ends[2:3, cols] = gain[cols].reshape(1, 128)
    lane = lax.broadcasted_iota(jnp.int32, (8, 128), 1)
    length = own.shape[0]

    @pl.when(place < EARLY)
    def _():
        ahead, behind, weight = ends[0:1, :], ends[1:2, :], ends[2:3, :]
        sums = jnp.zeros((8, 128), jnp.float32)
        for i in range(length // 8):
            rows = slice(8 * i, 8 * i + 8)
            value = own[rows, :] + first[rows, :] * ahead + second[rows, :] * behind
            gated[rows, :] = value * weight
            part = jnp.sum(value * value, axis=1, keepdims=True)
            sums = jnp.where(lane == i, part, sums)
        total_sum[...] = sums

    @pl.when(place >= EARLY)
    def _():
        lower, upper = triangle(length, False), triangle(length, True)
        squares = jnp.zeros((length, 128), jnp.float32)
        for at, width in CHUNKS:
            cols = pl.ds(at, width)
            down, up, mine, rest, share = local_parts(
                total, lower, upper, fade, push, gate, cols
            )
            value = (down * (mine + ends[0:1, cols]) + up * (rest + ends[1:2, cols])) * share
            gated[:, cols] = value * ends[2:3, cols]
            value = value * value
            for k in range(width // 128):
                squares = squares + value[:, 128 * k : 128 * k + 128]
        sums = jnp.zeros((8, 128), jnp.float32)
        for i in range(length // 8):
            part = jnp.sum(squares[8 * i : 8 * i + 8, :], axis=1, keepdims=True)
            sums = jnp.where(lane == i, part, sums)
        total_sum[...] = sums

    for k in range(power.shape[0]):
        power[k] = total_sum[...]


def norm_kernel(channels, powers, gated, out_hbm, out, sems):
    power = powers[0] + powers[1] + powers[2] + powers[3]
    root = lax.rsqrt(power * (1.0 / channels) + 1e-06)
    count, pieces = out.shape[0] // 16, []
    for i in range(count):
        rows = slice(16 * i, 16 * i + 16)
        r = jnp.concatenate([root[:, 2 * i : 2 * i + 1], root[:, 2 * i + 1 : 2 * i + 2]], axis=0)
        out[rows, :] = (gated[rows, :] * r).astype(jnp.bfloat16)
        if (i + 1) % (count // PIECES) == 0:
            half = (i + 1) // (count // PIECES) - 1
            size = out.shape[0] // PIECES
            piece = pltpu.make_async_copy(
                out.at[pl.ds(half * size, size), :],
                out_hbm.at[pl.ds(half * size, size), :],
                sems.at[half],
            )
            piece.start()
            pieces.append(piece)
    for piece in pieces:
        piece.wait()


ANY = pl.BlockSpec(memory_space=pl.ANY)
HBM = pl.BlockSpec(memory_space=pltpu.HBM)
VMEM = pl.BlockSpec(memory_space=pltpu.VMEM)


def shape_of(*shape, dtype=jnp.float32):
    return jax.ShapeDtypeStruct(shape, dtype)


def in_hbm(value):
    return pltpu.with_memory_space_constraint(value, pltpu.HBM)


def per_device(fade_rate, update_in, gate_in, norm_gain):
    fade_rate, update_in, gate_in = fade_rate[0], update_in[0], gate_in[0]
    length, width = fade_rate.shape
    chips, chans = lax.axis_size("z"), lax.axis_size("chan")
    total = float(length * chips * lax.axis_size("core"))
    params = pltpu.CompilerParams(vmem_limit_bytes=16 * 2**20)
    f32, bf16 = jnp.float32, jnp.bfloat16
    block = (length, width)
    summary, fade, push, gate, gain = pl.pallas_call(
        functools.partial(summary_kernel, total),
        out_shape=[
            shape_of(3, width),
            shape_of(*block),
            shape_of(*block, dtype=bf16),
            shape_of(*block, dtype=bf16),
            shape_of(width),
        ],
        in_specs=[HBM] * 4,
        out_specs=[VMEM] * 5,
        scratch_shapes=[
            pltpu.SemaphoreType.DMA((len(CHUNKS), 2)),
            pltpu.SemaphoreType.DMA((2,)),
        ],
        compiler_params=params,
        name="summary",
    )(in_hbm(fade_rate), in_hbm(update_in), in_hbm(gate_in), in_hbm(norm_gain))
    both = lax.all_gather(summary, "core")
    sent, own, first, second = pl.pallas_call(
        functools.partial(chip_kernel, total),
        out_shape=[shape_of(chips, 2, width)] + [shape_of(*block)] * 3,
        in_specs=[VMEM] * 4,
        out_specs=[VMEM] * 4,
        compiler_params=params,
        name="chip",
    )(both, fade, push, gate)
    groups = [[2 * z + (c if z in NEAR else 1 - c) for z in ORDER] for c in (0, 1)]
    others = lax.all_to_all(sent, ("z", "core"), 0, 0, axis_index_groups=groups, tiled=True)
    gated, power = pl.pallas_call(
        functools.partial(join_kernel, total),
        out_shape=[shape_of(*block), shape_of(chans, 8, 128)],
        in_specs=[VMEM] * 9,
        out_specs=[VMEM] * 2,
        scratch_shapes=[pltpu.VMEM((3, width), f32), pltpu.VMEM((8, 128), f32)],
        compiler_params=params,
        name="join",
    )(both, others, fade, push, gate, own, first, second, gain)
    powers = lax.all_to_all(
        power, "chan", 0, 0, axis_index_groups=[list(CHAN_ORDER)], tiled=True
    )
    out = pl.pallas_call(
        functools.partial(norm_kernel, float(width * chans)),
        out_shape=shape_of(*block, dtype=bf16),
        in_specs=[VMEM] * 2,
        out_specs=ANY,
        scratch_shapes=[pltpu.VMEM(block, bf16), pltpu.SemaphoreType.DMA((PIECES,))],
        compiler_params=params,
        name="norm",
    )(powers, gated)
    return out[None]


def solution(mesh):
    torus = Mesh(
        mesh.devices.reshape(mesh.shape["trial"], mesh.shape["time"] // 2, 2, mesh.shape["chan"]),
        ("trial", "z", "core", "chan"),
    )
    time = ("z", "core")
    spec = P("trial", time, "chan")
    return jax.shard_map(
        per_device,
        mesh=torus,
        in_specs=(spec, spec, spec, P(("trial", "chan"))),
        out_specs=spec,
        check_vma=False,
    )
```

```python
import functools

import jax
import jax.numpy as jnp
from jax import lax
from jax.experimental import pallas as pl
from jax.experimental.pallas import tpu as pltpu
from jax.sharding import Mesh
from jax.sharding import PartitionSpec as P

CHUNKS = ((0, 384), (384, 256))
ORDER = (11, 12, 13, 14, 15, 0, 1, 2, 3, 4, 5, 6, 7, 8, 9, 10)
PIECES = 4
CHAN_ORDER = (2, 1, 0, 3)
EARLY = 3
NEAR = (0, 1)


def dot_split(left, right):
    high = right.astype(jnp.bfloat16)
    low = (right - high.astype(jnp.float32)).astype(jnp.bfloat16)
    return jnp.dot(left, high, preferred_element_type=jnp.float32) + jnp.dot(
        left, low, preferred_element_type=jnp.float32
    )


def triangle(size, upper):
    row = lax.broadcasted_iota(jnp.int32, (size, size), 0)
    col = lax.broadcasted_iota(jnp.int32, (size, size), 1)
    keep = (col >= row) if upper else (col <= row)
    return keep.astype(jnp.float32).astype(jnp.bfloat16)


def copies(sources, targets, sems):
    rows = []
    for k, (at, width) in enumerate(CHUNKS):
        rows.append(
            [
                pltpu.make_async_copy(
                    s.at[:, pl.ds(at, width)], t.at[:, pl.ds(at, width)], sems.at[k, n]
                )
                for n, (s, t) in enumerate(zip(sources, targets))
            ]
        )
    for row in rows:
        for copy in row:
            copy.start()
    return rows


def summary_kernel(
    total, fade_hbm, push_hbm, gate_hbm, gain_hbm, out, fade, push, gate, gain, sems, late_sems
):
    rows = copies((fade_hbm, push_hbm), (fade, push), sems)
    late = [
        pltpu.make_async_copy(gate_hbm, gate, late_sems.at[0]),
        pltpu.make_async_copy(gain_hbm, gain, late_sems.at[1]),
    ]
    for copy in late:
        copy.start()
    lower = triangle(fade.shape[0], False)
    for (at, width), row in zip(CHUNKS, rows):
        for copy in row:
            copy.wait()
        cols = pl.ds(at, width)
        rate = fade[:, cols] * (1.0 / total)
        value = push[:, cols].astype(jnp.float32)
        run = dot_split(lower, rate)
        all_of = jnp.sum(rate, axis=0, keepdims=True)
        product = jnp.exp(-all_of)
        scale = total ** (-0.5)
        out[0:1, cols] = product
        out[1:2, cols] = (
            product * scale * jnp.sum(jnp.exp(run) * value, axis=0, keepdims=True)
        )
        out[2:3, cols] = scale * jnp.sum(jnp.exp(rate - run) * value, axis=0, keepdims=True)
    for copy in late:
        copy.wait()


def local_parts(total, lower, upper, fade, push, gate, cols):
    rate = fade[:, cols] * (1.0 / total)
    value = push[:, cols].astype(jnp.float32) * total ** (-0.5)
    run = dot_split(lower, rate)
    down = jnp.exp(-run)
    up = jnp.exp(run - rate)
    ahead = dot_split(lower, jnp.exp(run) * value)
    behind = dot_split(upper, jnp.exp(rate - run) * value)
    share = 1.0 / (1.0 + jnp.exp(-gate[:, cols].astype(jnp.float32)))
    return down, up, ahead, behind, share


def chip_kernel(total, both, fade, push, gate, out, own, first, second):
    place = lax.axis_index("z")
    p0, f0, b0 = (both[0, k : k + 1, :] for k in range(3))
    p1, f1, b1 = (both[1, k : k + 1, :] for k in range(3))
    product = p0 * p1
    forward = f1 + p1 * f0
    backward = b0 + p0 * b1
    count = out.shape[0]
    for k in range(count):
        out[k, 0:1, :] = product
        out[k, 1:2, :] = jnp.where(place < ORDER[k], forward, backward)

    @pl.when(place < EARLY)
    def _():
        lower, upper = triangle(fade.shape[0], False), triangle(fade.shape[0], True)
        for at, width in CHUNKS:
            cols = pl.ds(at, width)
            down, up, ahead, behind, share = local_parts(
                total, lower, upper, fade, push, gate, cols
            )
            first[:, cols] = down * share
            second[:, cols] = up * share
            own[:, cols] = (down * ahead + up * behind) * share


def join_kernel(
    total, both, others, fade, push, gate, own, first, second, gain, gated, power, ends, total_sum
):
    place, core = lax.axis_index("z"), lax.axis_index("core")
    count = others.shape[0]
    ahead = jnp.zeros_like(both[0, 0:1, :])
    behind = jnp.zeros_like(ahead)
    for k in range(count):
        at = ORDER.index(k)
        ahead = jnp.where(k < place, others[at, 0:1, :] * ahead + others[at, 1:2, :], ahead)
        j = count - 1 - k
        at = ORDER.index(j)
        behind = jnp.where(j > place, others[at, 0:1, :] * behind + others[at, 1:2, :], behind)
    p0, f0 = both[0, 0:1, :], both[0, 1:2, :]
    p1, b1 = both[1, 0:1, :], both[1, 2:3, :]
    low = core == 0
    ends[0:1, :] = jnp.where(low, ahead, f0 + p0 * ahead)
    ends[1:2, :] = jnp.where(low, p0 * (b1 + p1 * behind), p1 * behind)
    for k in range(gain.shape[0] // 128):
        cols = pl.ds(128 * k, 128)
        ends[2:3, cols] = gain[cols].reshape(1, 128)
    lane = lax.broadcasted_iota(jnp.int32, (8, 128), 1)
    length = own.shape[0]

    @pl.when(place < EARLY)
    def _():
        ahead, behind, weight = ends[0:1, :], ends[1:2, :], ends[2:3, :]
        sums = jnp.zeros((8, 128), jnp.float32)
        for i in range(length // 8):
            rows = slice(8 * i, 8 * i + 8)
            value = own[rows, :] + first[rows, :] * ahead + second[rows, :] * behind
            gated[rows, :] = value * weight
            part = jnp.sum(value * value, axis=1, keepdims=True)
            sums = jnp.where(lane == i, part, sums)
        total_sum[...] = sums

    @pl.when(place >= EARLY)
    def _():
        lower, upper = triangle(length, False), triangle(length, True)
        squares = jnp.zeros((length, 128), jnp.float32)
        for at, width in CHUNKS:
            cols = pl.ds(at, width)
            down, up, mine, rest, share = local_parts(
                total, lower, upper, fade, push, gate, cols
            )
            value = (down * (mine + ends[0:1, cols]) + up * (rest + ends[1:2, cols])) * share
            gated[:, cols] = value * ends[2:3, cols]
            value = value * value
            for k in range(width // 128):
                squares = squares + value[:, 128 * k : 128 * k + 128]
        sums = jnp.zeros((8, 128), jnp.float32)
        for i in range(length // 8):
            part = jnp.sum(squares[8 * i : 8 * i + 8, :], axis=1, keepdims=True)
            sums = jnp.where(lane == i, part, sums)
        total_sum[...] = sums

    for k in range(power.shape[0]):
        power[k] = total_sum[...]


def norm_kernel(channels, powers, gated, out_hbm, out, sems):
    power = powers[0] + powers[1] + powers[2] + powers[3]
    root = lax.rsqrt(power * (1.0 / channels) + 1e-06)
    count, pieces = out.shape[0] // 16, []
    for i in range(count):
        rows = slice(16 * i, 16 * i + 16)
        r = jnp.concatenate([root[:, 2 * i : 2 * i + 1], root[:, 2 * i + 1 : 2 * i + 2]], axis=0)
        out[rows, :] = (gated[rows, :] * r).astype(jnp.bfloat16)
        if (i + 1) % (count // PIECES) == 0:
            half = (i + 1) // (count // PIECES) - 1
            size = out.shape[0] // PIECES
            piece = pltpu.make_async_copy(
                out.at[pl.ds(half * size, size), :],
                out_hbm.at[pl.ds(half * size, size), :],
                sems.at[half],
            )
            piece.start()
            pieces.append(piece)
    for piece in pieces:
        piece.wait()


ANY = pl.BlockSpec(memory_space=pl.ANY)
HBM = pl.BlockSpec(memory_space=pltpu.HBM)
VMEM = pl.BlockSpec(memory_space=pltpu.VMEM)


def shape_of(*shape, dtype=jnp.float32):
    return jax.ShapeDtypeStruct(shape, dtype)


def in_hbm(value):
    return pltpu.with_memory_space_constraint(value, pltpu.HBM)


def per_device(fade_rate, update_in, gate_in, norm_gain):
    fade_rate, update_in, gate_in = fade_rate[0], update_in[0], gate_in[0]
    length, width = fade_rate.shape
    chips, chans = lax.axis_size("z"), lax.axis_size("chan")
    total = float(length * chips * lax.axis_size("core"))
    params = pltpu.CompilerParams(vmem_limit_bytes=16 * 2**20)
    f32, bf16 = jnp.float32, jnp.bfloat16
    block = (length, width)
    summary, fade, push, gate, gain = pl.pallas_call(
        functools.partial(summary_kernel, total),
        out_shape=[
            shape_of(3, width),
            shape_of(*block),
            shape_of(*block, dtype=bf16),
            shape_of(*block, dtype=bf16),
            shape_of(width),
        ],
        in_specs=[HBM] * 4,
        out_specs=[VMEM] * 5,
        scratch_shapes=[
            pltpu.SemaphoreType.DMA((len(CHUNKS), 2)),
            pltpu.SemaphoreType.DMA((2,)),
        ],
        compiler_params=params,
        name="summary",
    )(in_hbm(fade_rate), in_hbm(update_in), in_hbm(gate_in), in_hbm(norm_gain))
    both = lax.all_gather(summary, "core")
    sent, own, first, second = pl.pallas_call(
        functools.partial(chip_kernel, total),
        out_shape=[shape_of(chips, 2, width)] + [shape_of(*block)] * 3,
        in_specs=[VMEM] * 4,
        out_specs=[VMEM] * 4,
        compiler_params=params,
        name="chip",
    )(both, fade, push, gate)
    groups = [[2 * z + (c if z in NEAR else 1 - c) for z in ORDER] for c in (0, 1)]
    others = lax.all_to_all(sent, ("z", "core"), 0, 0, axis_index_groups=groups, tiled=True)
    gated, power = pl.pallas_call(
        functools.partial(join_kernel, total),
        out_shape=[shape_of(*block), shape_of(chans, 8, 128)],
        in_specs=[VMEM] * 9,
        out_specs=[VMEM] * 2,
        scratch_shapes=[pltpu.VMEM((3, width), f32), pltpu.VMEM((8, 128), f32)],
        compiler_params=params,
        name="join",
    )(both, others, fade, push, gate, own, first, second, gain)
    powers = lax.all_to_all(
        power, "chan", 0, 0, axis_index_groups=[list(CHAN_ORDER)], tiled=True
    )
    out = pl.pallas_call(
        functools.partial(norm_kernel, float(width * chans)),
        out_shape=shape_of(*block, dtype=bf16),
        in_specs=[VMEM] * 2,
        out_specs=ANY,
        scratch_shapes=[pltpu.VMEM(block, bf16), pltpu.SemaphoreType.DMA((PIECES,))],
        compiler_params=params,
        name="norm",
    )(powers, gated)
    return out[None]


def solution(mesh):
    torus = Mesh(
        mesh.devices.reshape(mesh.shape["trial"], mesh.shape["time"] // 2, 2, mesh.shape["chan"]),
        ("trial", "z", "core", "chan"),
    )
    time = ("z", "core")
    spec = P("trial", time, "chan")
    return jax.shard_map(
        per_device,
        mesh=torus,
        in_specs=(spec, spec, spec, P(("trial", "chan"))),
        out_specs=spec,
        check_vma=False,
    )
```

```python
import functools

import jax
import jax.numpy as jnp
from jax import lax
from jax.experimental import pallas as pl
from jax.experimental.pallas import tpu as pltpu
from jax.sharding import Mesh
from jax.sharding import PartitionSpec as P

CHUNKS = ((0, 384), (384, 256))
ORDER = (11, 12, 13, 14, 15, 0, 1, 2, 3, 4, 5, 6, 7, 8, 9, 10)
PIECES = 4
CHAN_ORDER = (2, 1, 0, 3)
EARLY = 3
NEAR = (0, 1, 2)


def dot_split(left, right):
    high = right.astype(jnp.bfloat16)
    low = (right - high.astype(jnp.float32)).astype(jnp.bfloat16)
    return jnp.dot(left, high, preferred_element_type=jnp.float32) + jnp.dot(
        left, low, preferred_element_type=jnp.float32
    )


def triangle(size, upper):
    row = lax.broadcasted_iota(jnp.int32, (size, size), 0)
    col = lax.broadcasted_iota(jnp.int32, (size, size), 1)
    keep = (col >= row) if upper else (col <= row)
    return keep.astype(jnp.float32).astype(jnp.bfloat16)


def copies(sources, targets, sems):
    rows = []
    for k, (at, width) in enumerate(CHUNKS):
        rows.append(
            [
                pltpu.make_async_copy(
                    s.at[:, pl.ds(at, width)], t.at[:, pl.ds(at, width)], sems.at[k, n]
                )
                for n, (s, t) in enumerate(zip(sources, targets))
            ]
        )
    for row in rows:
        for copy in row:
            copy.start()
    return rows


def summary_kernel(
    total, fade_hbm, push_hbm, gate_hbm, gain_hbm, out, fade, push, gate, gain, sems, late_sems
):
    rows = copies((fade_hbm, push_hbm), (fade, push), sems)
    late = [
        pltpu.make_async_copy(gate_hbm, gate, late_sems.at[0]),
        pltpu.make_async_copy(gain_hbm, gain, late_sems.at[1]),
    ]
    for copy in late:
        copy.start()
    lower = triangle(fade.shape[0], False)
    for (at, width), row in zip(CHUNKS, rows):
        for copy in row:
            copy.wait()
        cols = pl.ds(at, width)
        rate = fade[:, cols] * (1.0 / total)
        value = push[:, cols].astype(jnp.float32)
        run = dot_split(lower, rate)
        all_of = jnp.sum(rate, axis=0, keepdims=True)
        product = jnp.exp(-all_of)
        scale = total ** (-0.5)
        out[0:1, cols] = product
        out[1:2, cols] = (
            product * scale * jnp.sum(jnp.exp(run) * value, axis=0, keepdims=True)
        )
        out[2:3, cols] = scale * jnp.sum(jnp.exp(rate - run) * value, axis=0, keepdims=True)
    for copy in late:
        copy.wait()


def local_parts(total, lower, upper, fade, push, gate, cols):
    rate = fade[:, cols] * (1.0 / total)
    value = push[:, cols].astype(jnp.float32) * total ** (-0.5)
    run = dot_split(lower, rate)
    down = jnp.exp(-run)
    up = jnp.exp(run - rate)
    ahead = dot_split(lower, jnp.exp(run) * value)
    behind = dot_split(upper, jnp.exp(rate - run) * value)
    share = 1.0 / (1.0 + jnp.exp(-gate[:, cols].astype(jnp.float32)))
    return down, up, ahead, behind, share


def chip_kernel(total, both, fade, push, gate, out, own, first, second):
    place = lax.axis_index("z")
    p0, f0, b0 = (both[0, k : k + 1, :] for k in range(3))
    p1, f1, b1 = (both[1, k : k + 1, :] for k in range(3))
    product = p0 * p1
    forward = f1 + p1 * f0
    backward = b0 + p0 * b1
    count = out.shape[0]
    for k in range(count):
        out[k, 0:1, :] = product
        out[k, 1:2, :] = jnp.where(place < ORDER[k], forward, backward)

    @pl.when(place < EARLY)
    def _():
        lower, upper = triangle(fade.shape[0], False), triangle(fade.shape[0], True)
        for at, width in CHUNKS:
            cols = pl.ds(at, width)
            down, up, ahead, behind, share = local_parts(
                total, lower, upper, fade, push, gate, cols
            )
            first[:, cols] = down * share
            second[:, cols] = up * share
            own[:, cols] = (down * ahead + up * behind) * share


def join_kernel(
    total, both, others, fade, push, gate, own, first, second, gain, gated, power, ends, total_sum
):
    place, core = lax.axis_index("z"), lax.axis_index("core")
    count = others.shape[0]
    ahead = jnp.zeros_like(both[0, 0:1, :])
    behind = jnp.zeros_like(ahead)
    for k in range(count):
        j = count - 1 - k
        at, back = ORDER.index(k), ORDER.index(j)
        decay = jnp.where(k < place, others[at, 0:1, :], 1.0)
        ahead = decay * ahead + jnp.where(k < place, others[at, 1:2, :], 0.0)
        decay = jnp.where(j > place, others[back, 0:1, :], 1.0)
        behind = decay * behind + jnp.where(j > place, others[back, 1:2, :], 0.0)
    p0, f0 = both[0, 0:1, :], both[0, 1:2, :]
    p1, b1 = both[1, 0:1, :], both[1, 2:3, :]
    low = core == 0
    ends[0:1, :] = jnp.where(low, ahead, f0 + p0 * ahead)
    ends[1:2, :] = jnp.where(low, p0 * (b1 + p1 * behind), p1 * behind)
    for k in range(gain.shape[0] // 128):
        cols = pl.ds(128 * k, 128)
        ends[2:3, cols] = gain[cols].reshape(1, 128)
    lane = lax.broadcasted_iota(jnp.int32, (8, 128), 1)
    length = own.shape[0]

    @pl.when(place < EARLY)
    def _():
        ahead, behind, weight = ends[0:1, :], ends[1:2, :], ends[2:3, :]
        sums = jnp.zeros((8, 128), jnp.float32)
        for i in range(length // 8):
            rows = slice(8 * i, 8 * i + 8)
            value = own[rows, :] + first[rows, :] * ahead + second[rows, :] * behind
            gated[rows, :] = value * weight
            part = jnp.sum(value * value, axis=1, keepdims=True)
            sums = jnp.where(lane == i, part, sums)
        total_sum[...] = sums

    @pl.when(place >= EARLY)
    def _():
        lower, upper = triangle(length, False), triangle(length, True)
        squares = jnp.zeros((length, 128), jnp.float32)
        for at, width in CHUNKS:
            cols = pl.ds(at, width)
            down, up, mine, rest, share = local_parts(
                total, lower, upper, fade, push, gate, cols
            )
            value = (down * (mine + ends[0:1, cols]) + up * (rest + ends[1:2, cols])) * share
            gated[:, cols] = value * ends[2:3, cols]
            value = value * value
            for k in range(width // 128):
                squares = squares + value[:, 128 * k : 128 * k + 128]
        sums = jnp.zeros((8, 128), jnp.float32)
        for i in range(length // 8):
            part = jnp.sum(squares[8 * i : 8 * i + 8, :], axis=1, keepdims=True)
            sums = jnp.where(lane == i, part, sums)
        total_sum[...] = sums

    for k in range(power.shape[0]):
        power[k] = total_sum[...]


def norm_kernel(channels, powers, gated, out_hbm, out, sems):
    power = powers[0] + powers[1] + powers[2] + powers[3]
    root = lax.rsqrt(power * (1.0 / channels) + 1e-06)
    count, pieces = out.shape[0] // 16, []
    for i in range(count):
        rows = slice(16 * i, 16 * i + 16)
        r = jnp.concatenate([root[:, 2 * i : 2 * i + 1], root[:, 2 * i + 1 : 2 * i + 2]], axis=0)
        out[rows, :] = (gated[rows, :] * r).astype(jnp.bfloat16)
        if (i + 1) % (count // PIECES) == 0:
            half = (i + 1) // (count // PIECES) - 1
            size = out.shape[0] // PIECES
            piece = pltpu.make_async_copy(
                out.at[pl.ds(half * size, size), :],
                out_hbm.at[pl.ds(half * size, size), :],
                sems.at[half],
            )
            piece.start()
            pieces.append(piece)
    for piece in pieces:
        piece.wait()


ANY = pl.BlockSpec(memory_space=pl.ANY)
HBM = pl.BlockSpec(memory_space=pltpu.HBM)
VMEM = pl.BlockSpec(memory_space=pltpu.VMEM)


def shape_of(*shape, dtype=jnp.float32):
    return jax.ShapeDtypeStruct(shape, dtype)


def in_hbm(value):
    return pltpu.with_memory_space_constraint(value, pltpu.HBM)


def per_device(fade_rate, update_in, gate_in, norm_gain):
    fade_rate, update_in, gate_in = fade_rate[0], update_in[0], gate_in[0]
    length, width = fade_rate.shape
    chips, chans = lax.axis_size("z"), lax.axis_size("chan")
    total = float(length * chips * lax.axis_size("core"))
    params = pltpu.CompilerParams(vmem_limit_bytes=16 * 2**20)
    f32, bf16 = jnp.float32, jnp.bfloat16
    block = (length, width)
    summary, fade, push, gate, gain = pl.pallas_call(
        functools.partial(summary_kernel, total),
        out_shape=[
            shape_of(3, width),
            shape_of(*block),
            shape_of(*block, dtype=bf16),
            shape_of(*block, dtype=bf16),
            shape_of(width),
        ],
        in_specs=[HBM] * 4,
        out_specs=[VMEM] * 5,
        scratch_shapes=[
            pltpu.SemaphoreType.DMA((len(CHUNKS), 2)),
            pltpu.SemaphoreType.DMA((2,)),
        ],
        compiler_params=params,
        name="summary",
    )(in_hbm(fade_rate), in_hbm(update_in), in_hbm(gate_in), in_hbm(norm_gain))
    both = lax.all_gather(summary, "core")
    sent, own, first, second = pl.pallas_call(
        functools.partial(chip_kernel, total),
        out_shape=[shape_of(chips, 2, width)] + [shape_of(*block)] * 3,
        in_specs=[VMEM] * 4,
        out_specs=[VMEM] * 4,
        compiler_params=params,
        name="chip",
    )(both, fade, push, gate)
    groups = [[2 * z + (c if z in NEAR else 1 - c) for z in ORDER] for c in (0, 1)]
    others = lax.all_to_all(sent, ("z", "core"), 0, 0, axis_index_groups=groups, tiled=True)
    gated, power = pl.pallas_call(
        functools.partial(join_kernel, total),
        out_shape=[shape_of(*block), shape_of(chans, 8, 128)],
        in_specs=[VMEM] * 9,
        out_specs=[VMEM] * 2,
        scratch_shapes=[pltpu.VMEM((3, width), f32), pltpu.VMEM((8, 128), f32)],
        compiler_params=params,
        name="join",
    )(both, others, fade, push, gate, own, first, second, gain)
    powers = lax.all_to_all(
        power, "chan", 0, 0, axis_index_groups=[list(CHAN_ORDER)], tiled=True
    )
    out = pl.pallas_call(
        functools.partial(norm_kernel, float(width * chans)),
        out_shape=shape_of(*block, dtype=bf16),
        in_specs=[VMEM] * 2,
        out_specs=ANY,
        scratch_shapes=[pltpu.VMEM(block, bf16), pltpu.SemaphoreType.DMA((PIECES,))],
        compiler_params=params,
        name="norm",
    )(powers, gated)
    return out[None]


def solution(mesh):
    torus = Mesh(
        mesh.devices.reshape(mesh.shape["trial"], mesh.shape["time"] // 2, 2, mesh.shape["chan"]),
        ("trial", "z", "core", "chan"),
    )
    time = ("z", "core")
    spec = P("trial", time, "chan")
    return jax.shard_map(
        per_device,
        mesh=torus,
        in_specs=(spec, spec, spec, P(("trial", "chan"))),
        out_specs=spec,
        check_vma=False,
    )
```

```python
import functools

import jax
import jax.numpy as jnp
from jax import lax
from jax.experimental import pallas as pl
from jax.experimental.pallas import tpu as pltpu
from jax.sharding import Mesh
from jax.sharding import PartitionSpec as P

CHUNKS = ((0, 384), (384, 256))
ORDER = (11, 12, 13, 14, 15, 0, 1, 2, 3, 4, 5, 6, 7, 8, 9, 10)
PIECES = 4
CHAN_ORDER = (2, 1, 0, 3)
EARLY = 3
NEAR = (0, 1, 2, 8)


def dot_split(left, right):
    high = right.astype(jnp.bfloat16)
    low = (right - high.astype(jnp.float32)).astype(jnp.bfloat16)
    return jnp.dot(left, high, preferred_element_type=jnp.float32) + jnp.dot(
        left, low, preferred_element_type=jnp.float32
    )


def triangle(size, upper):
    row = lax.broadcasted_iota(jnp.int32, (size, size), 0)
    col = lax.broadcasted_iota(jnp.int32, (size, size), 1)
    keep = (col >= row) if upper else (col <= row)
    return keep.astype(jnp.float32).astype(jnp.bfloat16)


def copies(sources, targets, sems):
    rows = []
    for k, (at, width) in enumerate(CHUNKS):
        rows.append(
            [
                pltpu.make_async_copy(
                    s.at[:, pl.ds(at, width)], t.at[:, pl.ds(at, width)], sems.at[k, n]
                )
                for n, (s, t) in enumerate(zip(sources, targets))
            ]
        )
    for row in rows:
        for copy in row:
            copy.start()
    return rows


def summary_kernel(
    total, fade_hbm, push_hbm, gate_hbm, gain_hbm, out, fade, push, gate, gain, sems, late_sems
):
    rows = copies((fade_hbm, push_hbm), (fade, push), sems)
    late = [
        pltpu.make_async_copy(gate_hbm, gate, late_sems.at[0]),
        pltpu.make_async_copy(gain_hbm, gain, late_sems.at[1]),
    ]
    for copy in late:
        copy.start()
    lower = triangle(fade.shape[0], False)
    for (at, width), row in zip(CHUNKS, rows):
        for copy in row:
            copy.wait()
        cols = pl.ds(at, width)
        rate = fade[:, cols] * (1.0 / total)
        value = push[:, cols].astype(jnp.float32)
        run = dot_split(lower, rate)
        all_of = jnp.sum(rate, axis=0, keepdims=True)
        product = jnp.exp(-all_of)
        scale = total ** (-0.5)
        out[0:1, cols] = product
        out[1:2, cols] = (
            product * scale * jnp.sum(jnp.exp(run) * value, axis=0, keepdims=True)
        )
        out[2:3, cols] = scale * jnp.sum(jnp.exp(rate - run) * value, axis=0, keepdims=True)
    for copy in late:
        copy.wait()


def local_parts(total, lower, upper, fade, push, gate, cols):
    rate = fade[:, cols] * (1.0 / total)
    value = push[:, cols].astype(jnp.float32) * total ** (-0.5)
    run = dot_split(lower, rate)
    down = jnp.exp(-run)
    up = jnp.exp(run - rate)
    ahead = dot_split(lower, jnp.exp(run) * value)
    behind = dot_split(upper, jnp.exp(rate - run) * value)
    share = 1.0 / (1.0 + jnp.exp(-gate[:, cols].astype(jnp.float32)))
    return down, up, ahead, behind, share


def chip_kernel(total, both, fade, push, gate, out, own, first, second):
    place = lax.axis_index("z")
    p0, f0, b0 = (both[0, k : k + 1, :] for k in range(3))
    p1, f1, b1 = (both[1, k : k + 1, :] for k in range(3))
    product = p0 * p1
    forward = f1 + p1 * f0
    backward = b0 + p0 * b1
    count = out.shape[0]
    for k in range(count):
        out[k, 0:1, :] = product
        out[k, 1:2, :] = jnp.where(place < ORDER[k], forward, backward)

    @pl.when(place < EARLY)
    def _():
        lower, upper = triangle(fade.shape[0], False), triangle(fade.shape[0], True)
        for at, width in CHUNKS:
            cols = pl.ds(at, width)
            down, up, ahead, behind, share = local_parts(
                total, lower, upper, fade, push, gate, cols
            )
            first[:, cols] = down * share
            second[:, cols] = up * share
            own[:, cols] = (down * ahead + up * behind) * share


def join_kernel(
    total, both, others, fade, push, gate, own, first, second, gain, gated, power, ends, total_sum
):
    place, core = lax.axis_index("z"), lax.axis_index("core")
    count = others.shape[0]
    ahead = jnp.zeros_like(both[0, 0:1, :])
    behind = jnp.zeros_like(ahead)
    for k in range(count):
        at = ORDER.index(k)
        ahead = jnp.where(k < place, others[at, 0:1, :] * ahead + others[at, 1:2, :], ahead)
        j = count - 1 - k
        at = ORDER.index(j)
        behind = jnp.where(j > place, others[at, 0:1, :] * behind + others[at, 1:2, :], behind)
    p0, f0 = both[0, 0:1, :], both[0, 1:2, :]
    p1, b1 = both[1, 0:1, :], both[1, 2:3, :]
    low = core == 0
    ends[0:1, :] = jnp.where(low, ahead, f0 + p0 * ahead)
    ends[1:2, :] = jnp.where(low, p0 * (b1 + p1 * behind), p1 * behind)
    for k in range(gain.shape[0] // 128):
        cols = pl.ds(128 * k, 128)
        ends[2:3, cols] = gain[cols].reshape(1, 128)
    lane = lax.broadcasted_iota(jnp.int32, (8, 128), 1)
    length = own.shape[0]

    @pl.when(place < EARLY)
    def _():
        ahead, behind, weight = ends[0:1, :], ends[1:2, :], ends[2:3, :]
        sums = jnp.zeros((8, 128), jnp.float32)
        for i in range(length // 8):
            rows = slice(8 * i, 8 * i + 8)
            value = own[rows, :] + first[rows, :] * ahead + second[rows, :] * behind
            gated[rows, :] = value * weight
            part = jnp.sum(value * value, axis=1, keepdims=True)
            sums = jnp.where(lane == i, part, sums)
        total_sum[...] = sums

    @pl.when(place >= EARLY)
    def _():
        lower, upper = triangle(length, False), triangle(length, True)
        squares = jnp.zeros((length, 128), jnp.float32)
        for at, width in CHUNKS:
            cols = pl.ds(at, width)
            down, up, mine, rest, share = local_parts(
                total, lower, upper, fade, push, gate, cols
            )
            value = (down * (mine + ends[0:1, cols]) + up * (rest + ends[1:2, cols])) * share
            gated[:, cols] = value * ends[2:3, cols]
            value = value * value
            for k in range(width // 128):
                squares = squares + value[:, 128 * k : 128 * k + 128]
        sums = jnp.zeros((8, 128), jnp.float32)
        for i in range(length // 8):
            part = jnp.sum(squares[8 * i : 8 * i + 8, :], axis=1, keepdims=True)
            sums = jnp.where(lane == i, part, sums)
        total_sum[...] = sums

    for k in range(power.shape[0]):
        power[k] = total_sum[...]


def norm_kernel(channels, powers, gated, out_hbm, out, sems):
    power = powers[0] + powers[1] + powers[2] + powers[3]
    root = lax.rsqrt(power * (1.0 / channels) + 1e-06)
    count, pieces = out.shape[0] // 16, []
    for i in range(count):
        rows = slice(16 * i, 16 * i + 16)
        r = jnp.concatenate([root[:, 2 * i : 2 * i + 1], root[:, 2 * i + 1 : 2 * i + 2]], axis=0)
        out[rows, :] = (gated[rows, :] * r).astype(jnp.bfloat16)
        if (i + 1) % (count // PIECES) == 0:
            half = (i + 1) // (count // PIECES) - 1
            size = out.shape[0] // PIECES
            piece = pltpu.make_async_copy(
                out.at[pl.ds(half * size, size), :],
                out_hbm.at[pl.ds(half * size, size), :],
                sems.at[half],
            )
            piece.start()
            pieces.append(piece)
    for piece in pieces:
        piece.wait()


ANY = pl.BlockSpec(memory_space=pl.ANY)
HBM = pl.BlockSpec(memory_space=pltpu.HBM)
VMEM = pl.BlockSpec(memory_space=pltpu.VMEM)


def shape_of(*shape, dtype=jnp.float32):
    return jax.ShapeDtypeStruct(shape, dtype)


def in_hbm(value):
    return pltpu.with_memory_space_constraint(value, pltpu.HBM)


def per_device(fade_rate, update_in, gate_in, norm_gain):
    fade_rate, update_in, gate_in = fade_rate[0], update_in[0], gate_in[0]
    length, width = fade_rate.shape
    chips, chans = lax.axis_size("z"), lax.axis_size("chan")
    total = float(length * chips * lax.axis_size("core"))
    params = pltpu.CompilerParams(vmem_limit_bytes=16 * 2**20)
    f32, bf16 = jnp.float32, jnp.bfloat16
    block = (length, width)
    summary, fade, push, gate, gain = pl.pallas_call(
        functools.partial(summary_kernel, total),
        out_shape=[
            shape_of(3, width),
            shape_of(*block),
            shape_of(*block, dtype=bf16),
            shape_of(*block, dtype=bf16),
            shape_of(width),
        ],
        in_specs=[HBM] * 4,
        out_specs=[VMEM] * 5,
        scratch_shapes=[
            pltpu.SemaphoreType.DMA((len(CHUNKS), 2)),
            pltpu.SemaphoreType.DMA((2,)),
        ],
        compiler_params=params,
        name="summary",
    )(in_hbm(fade_rate), in_hbm(update_in), in_hbm(gate_in), in_hbm(norm_gain))
    both = lax.all_gather(summary, "core")
    sent, own, first, second = pl.pallas_call(
        functools.partial(chip_kernel, total),
        out_shape=[shape_of(chips, 2, width)] + [shape_of(*block)] * 3,
        in_specs=[VMEM] * 4,
        out_specs=[VMEM] * 4,
        compiler_params=params,
        name="chip",
    )(both, fade, push, gate)
    groups = [[2 * z + (c if z in NEAR else 1 - c) for z in ORDER] for c in (0, 1)]
    others = lax.all_to_all(sent, ("z", "core"), 0, 0, axis_index_groups=groups, tiled=True)
    gated, power = pl.pallas_call(
        functools.partial(join_kernel, total),
        out_shape=[shape_of(*block), shape_of(chans, 8, 128)],
        in_specs=[VMEM] * 9,
        out_specs=[VMEM] * 2,
        scratch_shapes=[pltpu.VMEM((3, width), f32), pltpu.VMEM((8, 128), f32)],
        compiler_params=params,
        name="join",
    )(both, others, fade, push, gate, own, first, second, gain)
    powers = lax.all_to_all(
        power, "chan", 0, 0, axis_index_groups=[list(CHAN_ORDER)], tiled=True
    )
    out = pl.pallas_call(
        functools.partial(norm_kernel, float(width * chans)),
        out_shape=shape_of(*block, dtype=bf16),
        in_specs=[VMEM] * 2,
        out_specs=ANY,
        scratch_shapes=[pltpu.VMEM(block, bf16), pltpu.SemaphoreType.DMA((PIECES,))],
        compiler_params=params,
        name="norm",
    )(powers, gated)
    return out[None]


def solution(mesh):
    torus = Mesh(
        mesh.devices.reshape(mesh.shape["trial"], mesh.shape["time"] // 2, 2, mesh.shape["chan"]),
        ("trial", "z", "core", "chan"),
    )
    time = ("z", "core")
    spec = P("trial", time, "chan")
    return jax.shard_map(
        per_device,
        mesh=torus,
        in_specs=(spec, spec, spec, P(("trial", "chan"))),
        out_specs=spec,
        check_vma=False,
    )
```
